32 devices in a mesh: wide: 16 (over z, y, core), narrow: 2 (over x).
Axes of the slice: x: 2, y: 2, z: 4, core: 2. Of those that a mesh axis runs over, the one named last changes fastest.
Arguments:
- query_coords: float32 [3, 32, 16, 32], P(None, ('wide', 'narrow')), may hold values from -1 to 1
- owner_element: int32 [32, 16, 32], P(('wide', 'narrow')), may hold values from 0 to 15
- pair_counts: int32 [32, 32], P(('wide', 'narrow')), may hold values from 0 to 16, as said below
- fields: bfloat16 [512, 8, 1024], P(('wide', 'narrow')), may hold values from -6 to 6
Outputs:
- values: bfloat16 [16, 32, 16, 32], P(None, ('wide', 'narrow'))
The draws below stay inside these ranges and needn't reach their ends.
Inputs may be any that keep to these rules, and one draw needn't show every extreme that they name: `pair_counts`: every count is at most 16, and some pair of devices reaches 16 in every draw.
All inputs are finite; a program needn't handle non-finite values.
Results may differ from the reference program's by a relative error of at most 0.0043.
Values may be sent and summed in bfloat16 or wider, within the bound.
No kernel may reach another device: no remote copies, remote signals or barrier semaphores. Data moves between devices by JAX's collectives and lax.ppermute only.
A program may use at most 64 MiB of HBM per device.

```python
import jax
import jax.numpy as jnp
from jax import lax

FIELDS = 16
NODE = 8
E_DEV = 16
CAP = 16
ELEMS = 512
DEVICES = 32


def draw_pair_counts(key, part):
    key_shift, key_hot, key_count, key_sender = jax.random.split(key, 4)
    shifts = jax.random.randint(key_shift, (DEVICES,), 0, 2)
    hottest = jax.random.randint(key_hot, (), 0, DEVICES)
    owners = jnp.arange(DEVICES)
    shifts = jnp.where(owners == hottest, 0, shifts)
    limits = jnp.maximum(jnp.right_shift(jnp.full((DEVICES,), CAP, jnp.int32), shifts.astype(jnp.int32)), 1)
    lowest = limits // 2
    raw_bits = jax.random.randint(key_count, (DEVICES, DEVICES), 0, 1 << 20)
    counts = lowest[None, :] + raw_bits % (limits[None, :] - lowest[None, :] + 1)
    sender = jax.random.randint(key_sender, (), 0, DEVICES)
    senders = jnp.arange(DEVICES)
    counts = jnp.where((senders[:, None] == sender) & (owners[None, :] == hottest), CAP, counts)
    return counts.astype(jnp.int32)


def with_ends(array, stream_key, low, high):
    spot = [jax.random.randint(jax.random.fold_in(stream_key, axis), (), 0, length) for axis, length in enumerate(array.shape)]
    longest = array.shape.index(max(array.shape))
    beside = spot[:longest] + [(spot[longest] + 1) % array.shape[longest]] + spot[longest + 1:]
    return array.at[tuple(spot)].set(low).at[tuple(beside)].set(high)


def shard_levels(own_key, extent, pieces, smallest, top_value):
    def one(axis_at, blocks):
        steps = jax.random.uniform(jax.random.fold_in(jax.random.fold_in(own_key, 6), axis_at), (blocks,), jnp.float32, smallest / len(pieces), top_value / len(pieces))
        return jnp.repeat(jnp.exp(steps), extent[axis_at] // blocks).reshape((-1,) + (1,) * (len(extent) - axis_at - 1))

    level = one(*pieces[0])
    for cut in pieces[1:]:
        level = level * one(*cut)
    return level


def centred(own_key, shape, spread, reach, cuts=(), kind=jnp.bfloat16):
    array = spread * jax.random.normal(own_key, shape, jnp.float32)
    if cuts:
        array = array * shard_levels(own_key, shape, cuts, -0.22, 0.18)
    return jnp.clip(array, -reach, reach).astype(kind)


def setup_inputs(seed: int = 0) -> dict:
    seeds = jax.random.split(jax.random.key(seed), 5)
    return {
        "query_coords": jnp.clip(jax.random.uniform(seeds[0], (3, DEVICES, CAP, DEVICES), jnp.float32, -1.0, 1.0) * shard_levels(seeds[0], (3, DEVICES, CAP, DEVICES), ((1, 32),), -0.4, 0.0), -1.0, 1.0),
        "owner_element": with_ends(jax.random.randint(seeds[1], (DEVICES, CAP, DEVICES), 0, E_DEV), jax.random.fold_in(seeds[1], 1), 0, E_DEV - 1).astype(jnp.int32),
        "pair_counts": draw_pair_counts(jax.random.fold_in(seeds[4], 71), 0),
        "fields": centred(seeds[3], (ELEMS, NODE, FIELDS * NODE * NODE), 1.0, 6.0, ((0, 32),)),
    }


GLL_NODES = (-1.0, -0.8717401485096066, -0.5917001814331423, -0.2092992179024789, 0.2092992179024789, 0.5917001814331423, 0.8717401485096066, 1.0)


def lagrange(position):
    result = []
    for i in range(8):
        factor = jnp.ones_like(position)
        for m in range(8):
            if m != i:
                factor = factor * ((position - GLL_NODES[m]) / (GLL_NODES[i] - GLL_NODES[m]))
        result.append(factor)
    return jnp.stack(result)


def reference(query_coords, owner_element, pair_counts, fields):
    field_table = fields.reshape(DEVICES, E_DEV, NODE, FIELDS * NODE * NODE)

    def one_owner(owner_index):
        coords_here = lax.dynamic_index_in_dim(query_coords, owner_index, 3, keepdims=False)
        element_here = lax.dynamic_index_in_dim(owner_element, owner_index, 2, keepdims=False)
        counts_here = lax.dynamic_index_in_dim(pair_counts, owner_index, 1, keepdims=False)
        owned = lax.dynamic_index_in_dim(field_table, owner_index, 0, keepdims=False)

        def one_slot(slot_index):
            picked_coords = lax.dynamic_index_in_dim(coords_here, slot_index, 2, keepdims=False)
            element_ids = lax.dynamic_index_in_dim(element_here, slot_index, 1, keepdims=False)
            live = slot_index < counts_here
            basis_r = lagrange(picked_coords[0]).astype(jnp.bfloat16).astype(jnp.float32)
            tensor_st = (lagrange(picked_coords[1])[:, None, :] * lagrange(picked_coords[2])[None, :, :]).reshape(NODE * NODE, -1)
            gathered = owned[element_ids].astype(jnp.float32)
            partial_value = jnp.einsum('sin,is->sn', gathered, basis_r)
            summed = jnp.sum(partial_value.reshape(-1, FIELDS, NODE * NODE) * tensor_st.T[:, None, :], axis=-1)
            return jnp.where(live[:, None], summed, jnp.float32(0.0)).astype(jnp.bfloat16).T

        return lax.map(one_slot, jnp.arange(CAP, dtype=jnp.int32))

    stacked = lax.map(one_owner, jnp.arange(DEVICES, dtype=jnp.int32))
    return jnp.transpose(stacked, (2, 3, 1, 0))
```

```python
import functools
import math

import jax
import jax.numpy as jnp
from jax import lax
from jax.experimental import pallas as pl
from jax.experimental.pallas import tpu as pltpu
from jax.sharding import PartitionSpec as P

GLL_NODES = (
    -1.0,
    -0.8717401485096066,
    -0.5917001814331423,
    -0.2092992179024789,
    0.2092992179024789,
    0.5917001814331423,
    0.8717401485096066,
    1.0,
)
NODE_COUNT = len(GLL_NODES)
SCALES = tuple(
    1.0 / math.prod(GLL_NODES[i] - GLL_NODES[m] for m in range(NODE_COUNT) if m != i)
    for i in range(NODE_COUNT)
)
AXES = ("wide", "narrow")
LANES = 128
ROWS = 8


def lagrange(position):
    node = lax.broadcasted_iota(jnp.int32, (NODE_COUNT, position.shape[1]), 0)
    result = jnp.full(node.shape, SCALES[0], jnp.float32)
    for i in range(1, NODE_COUNT):
        result = jnp.where(node == i, SCALES[i], result)
    for m in range(NODE_COUNT):
        result = result * jnp.where(node == m, 1.0, position - GLL_NODES[m])
    return result


def pack_kernel(coords_ref, element_ref, counts_ref, out_ref, *, element_count):
    slots, devices = element_ref.shape
    slot = lax.broadcasted_iota(jnp.int32, (slots, devices), 0)
    element = jnp.where(slot < counts_ref[...], element_ref[...], element_count)
    rows = jnp.concatenate(
        [
            coords_ref[...].reshape(3 * slots, devices),
            element.astype(jnp.float32),
            jnp.zeros(((ROWS - 4) * slots, devices), jnp.float32),
        ],
        axis=0,
    )
    out_ref[...] = rows.T


def evaluate_kernel(query_ref, fields_ref, out_ref, query_rows, result_rows, *, slots):
    senders = query_ref.shape[0]
    points = senders * slots
    table_rows, columns = fields_ref.shape
    element_count = table_rows // NODE_COUNT
    pairs = NODE_COUNT * NODE_COUNT
    field_count = columns // pairs
    query_rows[:, :senders] = query_ref[...].T
    query = jnp.concatenate(
        [query_rows[pl.ds(k, ROWS, stride=slots), :senders] for k in range(slots)], axis=1
    )
    basis_r = lagrange(query[0:1]).astype(jnp.bfloat16).astype(jnp.float32)
    basis_s = lagrange(query[1:2])
    basis_t = lagrange(query[2:3])
    element = query[3:4]
    weights = jnp.concatenate(
        [jnp.where(element == float(e), basis_r, 0.0) for e in range(element_count)], axis=0
    ).astype(jnp.bfloat16)
    tensor_st = jnp.concatenate(
        [basis_s[j : j + 1] * basis_t for j in range(NODE_COUNT)], axis=0
    )
    partial = lax.dot_general(
        fields_ref[...],
        weights,
        (((0,), (0,)), ((), ())),
        preferred_element_type=jnp.float32,
    )
    values = jnp.sum(
        partial.reshape(field_count, pairs, points) * tensor_st[None, :, :], axis=1
    )
    for k in range(slots):
        start = k * senders
        tile = values[:, start // LANES * LANES : start // LANES * LANES + LANES]
        shift = start % LANES
        if shift:
            tile = pltpu.roll(tile, LANES - shift, 1)
        result_rows[pl.ds(k, field_count, stride=slots), :] = tile
    out_ref[...] = result_rows[...].T[:senders].astype(jnp.bfloat16)


def unpack_kernel(result_ref, out_ref):
    out_ref[...] = (
        result_ref[...].astype(jnp.float32).T.reshape(out_ref.shape).astype(jnp.bfloat16)
    )


def exchange(array):
    return lax.all_to_all(array, AXES, split_axis=0, concat_axis=0, tiled=True)


def on_device(query_coords, owner_element, pair_counts, fields):
    device_count = lax.axis_size("wide") * lax.axis_size("narrow")
    slots = owner_element.shape[1]
    element_count, node_count, columns = fields.shape
    field_count = columns // (node_count * node_count)
    field_table = fields.reshape(element_count * node_count, columns)
    sent = pl.pallas_call(
        functools.partial(pack_kernel, element_count=element_count),
        out_shape=jax.ShapeDtypeStruct((device_count, ROWS * slots), jnp.float32),
        name="pack",
    )(query_coords[:, 0], owner_element[0], pair_counts)
    arrived = exchange(sent)
    senders = math.gcd(device_count, 32)
    result = pl.pallas_call(
        functools.partial(evaluate_kernel, slots=slots),
        out_shape=jax.ShapeDtypeStruct((device_count, field_count * slots), jnp.bfloat16),
        grid=(device_count // senders,),
        in_specs=[
            pl.BlockSpec((senders, ROWS * slots), lambda b: (b, 0)),
            pl.BlockSpec(field_table.shape, lambda b: (0, 0)),
        ],
        out_specs=pl.BlockSpec((senders, field_count * slots), lambda b: (b, 0)),
        scratch_shapes=[
            pltpu.VMEM((ROWS * slots, LANES), jnp.float32),
            pltpu.VMEM((field_count * slots, LANES), jnp.float32),
        ],
        name="evaluate",
    )(arrived, field_table)
    returned = exchange(result)
    values = pl.pallas_call(
        unpack_kernel,
        out_shape=jax.ShapeDtypeStruct((field_count, slots, device_count), jnp.bfloat16),
        name="unpack",
    )(returned)
    return values[:, None]


def solution(mesh):
    placed = (
        P(None, AXES, None, None),
        P(AXES, None, None),
        P(AXES, None),
        P(AXES, None, None),
    )
    return jax.shard_map(
        on_device,
        mesh=mesh,
        in_specs=placed,
        out_specs=P(None, AXES, None, None),
        check_vma=False,
    )
```

```python
import functools
import math

import jax
import jax.numpy as jnp
from jax import lax
from jax.experimental import pallas as pl
from jax.experimental.pallas import tpu as pltpu
from jax.sharding import PartitionSpec as P

GLL_NODES = (
    -1.0,
    -0.8717401485096066,
    -0.5917001814331423,
    -0.2092992179024789,
    0.2092992179024789,
    0.5917001814331423,
    0.8717401485096066,
    1.0,
)
NODE_COUNT = len(GLL_NODES)
SCALES = tuple(
    1.0 / math.prod(GLL_NODES[i] - GLL_NODES[m] for m in range(NODE_COUNT) if m != i)
    for i in range(NODE_COUNT)
)
AXES = ("wide", "narrow")
LANES = 128
ROWS = 8


def lagrange(position):
    node = lax.broadcasted_iota(jnp.int32, (NODE_COUNT, position.shape[1]), 0)
    result = jnp.full(node.shape, SCALES[0], jnp.float32)
    for i in range(1, NODE_COUNT):
        result = jnp.where(node == i, SCALES[i], result)
    for m in range(NODE_COUNT):
        result = result * jnp.where(node == m, 1.0, position - GLL_NODES[m])
    return result


def pack_kernel(coords_ref, element_ref, counts_ref, out_ref, *, element_count):
    slots, devices = element_ref.shape
    slot = lax.broadcasted_iota(jnp.int32, (slots, devices), 0)
    element = jnp.where(slot < counts_ref[...], element_ref[...], element_count)
    rows = jnp.concatenate(
        [
            coords_ref[...].reshape(3 * slots, devices),
            element.astype(jnp.float32),
            jnp.zeros(((ROWS - 4) * slots, devices), jnp.float32),
        ],
        axis=0,
    )
    out_ref[...] = rows.T


def evaluate_kernel(
    query_ref, fields_ref, out_ref, query_rows, result_rows, sent_rows, *, slots
):
    senders = query_ref.shape[0]
    points = senders * slots
    table_rows, columns = fields_ref.shape
    element_count = table_rows // NODE_COUNT
    pairs = NODE_COUNT * NODE_COUNT
    field_count = columns // pairs
    query_rows[:, :senders] = query_ref[...].T
    query = jnp.concatenate(
        [query_rows[pl.ds(k, ROWS, stride=slots), :senders] for k in range(slots)], axis=1
    )
    basis_r = lagrange(query[0:1]).astype(jnp.bfloat16).astype(jnp.float32)
    basis_s = lagrange(query[1:2])
    basis_t = lagrange(query[2:3])
    element = query[3:4]
    weights = jnp.concatenate(
        [jnp.where(element == float(e), basis_r, 0.0) for e in range(element_count)], axis=0
    ).astype(jnp.bfloat16)
    tensor_st = jnp.concatenate(
        [basis_s[j : j + 1] * basis_t for j in range(NODE_COUNT)], axis=0
    )
    partial = lax.dot_general(
        fields_ref[...],
        weights,
        (((0,), (0,)), ((), ())),
        preferred_element_type=jnp.float32,
    )
    values = jnp.sum(
        partial.reshape(field_count, pairs, points) * tensor_st[None, :, :], axis=1
    )
    for k in range(slots):
        start = k * senders
        tile = values[:, start // LANES * LANES : start // LANES * LANES + LANES]
        shift = start % LANES
        if shift:
            tile = pltpu.roll(tile, LANES - shift, 1)
        result_rows[pl.ds(k, field_count, stride=slots), :] = tile
    pieces = field_count * slots // LANES
    for piece in range(pieces):
        sent_rows[pl.ds(piece, senders, stride=pieces), :] = result_rows[
            piece * LANES : (piece + 1) * LANES, :
        ].T[:senders]
    out_ref[...] = sent_rows[...].astype(jnp.bfloat16)


def unpack_kernel(result_ref, out_ref, arrived_rows):
    field_count, slots, devices = out_ref.shape
    pieces = field_count * slots // LANES
    share = field_count // pieces
    arrived_rows[...] = result_ref[...].astype(jnp.float32)
    for piece in range(pieces):
        rows = arrived_rows[pl.ds(piece, devices, stride=pieces), :].T
        out_ref[piece * share : (piece + 1) * share] = rows.reshape(
            share, slots, devices
        ).astype(jnp.bfloat16)


def exchange(array):
    return lax.all_to_all(array, AXES, split_axis=0, concat_axis=0, tiled=True)


def on_device(query_coords, owner_element, pair_counts, fields):
    device_count = lax.axis_size("wide") * lax.axis_size("narrow")
    slots = owner_element.shape[1]
    element_count, node_count, columns = fields.shape
    field_count = columns // (node_count * node_count)
    field_table = fields.reshape(element_count * node_count, columns)
    sent = pl.pallas_call(
        functools.partial(pack_kernel, element_count=element_count),
        out_shape=jax.ShapeDtypeStruct((device_count, ROWS * slots), jnp.float32),
        name="pack",
    )(query_coords[:, 0], owner_element[0], pair_counts)
    arrived = exchange(sent)
    senders = math.gcd(device_count, 32)
    pieces = field_count * slots // LANES
    result = pl.pallas_call(
        functools.partial(evaluate_kernel, slots=slots),
        out_shape=jax.ShapeDtypeStruct((device_count * pieces, LANES), jnp.bfloat16),
        grid=(device_count // senders,),
        in_specs=[
            pl.BlockSpec((senders, ROWS * slots), lambda b: (b, 0)),
            pl.BlockSpec(field_table.shape, lambda b: (0, 0)),
        ],
        out_specs=pl.BlockSpec((senders * pieces, LANES), lambda b: (b, 0)),
        scratch_shapes=[
            pltpu.VMEM((ROWS * slots, LANES), jnp.float32),
            pltpu.VMEM((field_count * slots, LANES), jnp.float32),
            pltpu.VMEM((senders * pieces, LANES), jnp.float32),
        ],
        name="evaluate",
    )(arrived, field_table)
    returned = exchange(result)
    values = pl.pallas_call(
        unpack_kernel,
        out_shape=jax.ShapeDtypeStruct((field_count, slots, device_count), jnp.bfloat16),
        scratch_shapes=[pltpu.VMEM((device_count * pieces, LANES), jnp.float32)],
        name="unpack",
    )(returned)
    return values[:, None]


def solution(mesh):
    placed = (
        P(None, AXES, None, None),
        P(AXES, None, None),
        P(AXES, None),
        P(AXES, None, None),
    )
    return jax.shard_map(
        on_device,
        mesh=mesh,
        in_specs=placed,
        out_specs=P(None, AXES, None, None),
        check_vma=False,
    )
```

```python
import functools
import math

import jax
import jax.numpy as jnp
from jax import lax
from jax.experimental import pallas as pl
from jax.experimental.pallas import tpu as pltpu
from jax.sharding import PartitionSpec as P

GLL_NODES = (
    -1.0,
    -0.8717401485096066,
    -0.5917001814331423,
    -0.2092992179024789,
    0.2092992179024789,
    0.5917001814331423,
    0.8717401485096066,
    1.0,
)
NODE_COUNT = len(GLL_NODES)
SCALES = tuple(
    1.0 / math.prod(GLL_NODES[i] - GLL_NODES[m] for m in range(NODE_COUNT) if m != i)
    for i in range(NODE_COUNT)
)
AXES = ("wide", "narrow")
LANES = 128
ROWS = 8
TABLE_COPIES = 8


def lagrange(position):
    node = lax.broadcasted_iota(jnp.int32, (NODE_COUNT, position.shape[1]), 0)
    result = jnp.full(node.shape, SCALES[0], jnp.float32)
    for i in range(1, NODE_COUNT):
        result = jnp.where(node == i, SCALES[i], result)
    for m in range(NODE_COUNT):
        result = result * jnp.where(node == m, 1.0, position - GLL_NODES[m])
    return result


def pack_kernel(
    coords_hbm,
    element_hbm,
    counts_hbm,
    fields_hbm,
    out_ref,
    table_ref,
    coords_ref,
    element_ref,
    counts_ref,
    input_semaphores,
    table_semaphores,
    *,
    element_count,
):
    pairs = ((coords_hbm, coords_ref), (element_hbm, element_ref), (counts_hbm, counts_ref))
    input_copies = [
        pltpu.make_async_copy(source, target, input_semaphores.at[i])
        for i, (source, target) in enumerate(pairs)
    ]
    share = table_ref.shape[0] // TABLE_COPIES
    table_copies = [
        pltpu.make_async_copy(
            fields_hbm.at[pl.ds(i * share, share), :],
            table_ref.at[pl.ds(i * share, share), :],
            table_semaphores.at[i],
        )
        for i in range(TABLE_COPIES)
    ]
    for copy in input_copies + table_copies:
        copy.start()
    for copy in input_copies:
        copy.wait()
    slots, devices = element_ref.shape
    slot = lax.broadcasted_iota(jnp.int32, (slots, devices), 0)
    element = jnp.where(slot < counts_ref[...], element_ref[...], element_count)
    rows = jnp.concatenate(
        [
            coords_ref[...].reshape(3 * slots, devices),
            element.astype(jnp.float32),
            jnp.zeros(((ROWS - 4) * slots, devices), jnp.float32),
        ],
        axis=0,
    )
    out_ref[...] = rows.T
    for copy in table_copies:
        copy.wait()


def evaluate_kernel(
    query_ref, fields_ref, out_ref, query_rows, result_rows, sent_rows, *, senders, slots
):
    points = senders * slots
    table_rows, columns = fields_ref.shape
    element_count = table_rows // NODE_COUNT
    pairs = NODE_COUNT * NODE_COUNT
    field_count = columns // pairs

    def one_block(first):
        query_rows[:, :senders] = query_ref[pl.ds(first, senders), :].T
        query = jnp.concatenate(
            [query_rows[pl.ds(k, ROWS, stride=slots), :senders] for k in range(slots)], axis=1
        )
        basis_r = lagrange(query[0:1]).astype(jnp.bfloat16).astype(jnp.float32)
        basis_s = lagrange(query[1:2])
        basis_t = lagrange(query[2:3])
        element = query[3:4]
        weights = jnp.concatenate(
            [jnp.where(element == float(e), basis_r, 0.0) for e in range(element_count)], axis=0
        ).astype(jnp.bfloat16)
        tensor_st = jnp.concatenate(
            [basis_s[j : j + 1] * basis_t for j in range(NODE_COUNT)], axis=0
        )
        partial = lax.dot_general(
            fields_ref[...],
            weights,
            (((0,), (0,)), ((), ())),
            preferred_element_type=jnp.float32,
        )
        values = jnp.sum(
            partial.reshape(field_count, pairs, points) * tensor_st[None, :, :], axis=1
        )
        for k in range(slots):
            start = k * senders
            tile = values[:, start // LANES * LANES : start // LANES * LANES + LANES]
            shift = start % LANES
            if shift:
                tile = pltpu.roll(tile, LANES - shift, 1)
            result_rows[pl.ds(k, field_count, stride=slots), :] = tile
        pieces = field_count * slots // LANES
        for piece in range(pieces):
            sent_rows[pl.ds(piece, senders, stride=pieces), :] = result_rows[
                piece * LANES : (piece + 1) * LANES, :
            ].T[:senders]
        out_ref[pl.ds(first * pieces, senders * pieces), :] = sent_rows[...].astype(jnp.bfloat16)

    if query_ref.shape[0] == senders:
        one_block(0)
    else:

        @pl.loop(0, query_ref.shape[0] // senders)
        def _(block):
            one_block(pl.multiple_of(block * senders, senders))


def unpack_kernel(result_ref, out_ref, arrived_rows):
    field_count, slots, devices = out_ref.shape
    pieces = field_count * slots // LANES
    share = field_count // pieces
    arrived_rows[...] = result_ref[...].astype(jnp.float32)
    for piece in range(pieces):
        rows = arrived_rows[pl.ds(piece, devices, stride=pieces), :].T
        out_ref[piece * share : (piece + 1) * share] = rows.reshape(
            share, slots, devices
        ).astype(jnp.bfloat16)


def exchange(array):
    return lax.all_to_all(array, AXES, split_axis=0, concat_axis=0, tiled=True)


def in_vmem(array):
    return pltpu.with_memory_space_constraint(array, pltpu.VMEM)


def on_device(query_coords, owner_element, pair_counts, fields):
    device_count = lax.axis_size("wide") * lax.axis_size("narrow")
    slots = owner_element.shape[1]
    element_count, node_count, columns = fields.shape
    field_count = columns // (node_count * node_count)
    field_table = fields.reshape(element_count * node_count, columns)
    on_chip = pl.BlockSpec(memory_space=pltpu.VMEM)
    queries = (query_coords[:, 0], owner_element[0], pair_counts)
    sent, table = pl.pallas_call(
        functools.partial(pack_kernel, element_count=element_count),
        out_shape=(
            pltpu.VMEM((device_count, ROWS * slots), jnp.float32),
            pltpu.VMEM(field_table.shape, field_table.dtype),
        ),
        in_specs=[pl.BlockSpec(memory_space=pl.ANY)] * 4,
        out_specs=(on_chip, on_chip),
        scratch_shapes=[
            *(pltpu.VMEM(array.shape, array.dtype) for array in queries),
            pltpu.SemaphoreType.DMA((len(queries),)),
            pltpu.SemaphoreType.DMA((TABLE_COPIES,)),
        ],
        name="pack",
    )(*queries, field_table)
    arrived = exchange(sent)
    senders = math.gcd(device_count, 32)
    pieces = field_count * slots // LANES
    result = pl.pallas_call(
        functools.partial(evaluate_kernel, senders=senders, slots=slots),
        out_shape=pltpu.VMEM((device_count * pieces, LANES), jnp.bfloat16),
        in_specs=[on_chip, on_chip],
        out_specs=on_chip,
        scratch_shapes=[
            pltpu.VMEM((ROWS * slots, LANES), jnp.float32),
            pltpu.VMEM((field_count * slots, LANES), jnp.float32),
            pltpu.VMEM((senders * pieces, LANES), jnp.float32),
        ],
        name="evaluate",
    )(in_vmem(arrived), in_vmem(table))
    returned = exchange(result)
    values = pl.pallas_call(
        unpack_kernel,
        out_shape=jax.ShapeDtypeStruct((field_count, slots, device_count), jnp.bfloat16),
        in_specs=[on_chip],
        out_specs=on_chip,
        scratch_shapes=[pltpu.VMEM((device_count * pieces, LANES), jnp.float32)],
        name="unpack",
    )(in_vmem(returned))
    return values[:, None]


def solution(mesh):
    placed = (
        P(None, AXES, None, None),
        P(AXES, None, None),
        P(AXES, None),
        P(AXES, None, None),
    )
    return jax.shard_map(
        on_device,
        mesh=mesh,
        in_specs=placed,
        out_specs=P(None, AXES, None, None),
        check_vma=False,
    )
```

```python
import functools
import math

import jax
import jax.numpy as jnp
from jax import lax
from jax.experimental import pallas as pl
from jax.experimental.pallas import tpu as pltpu
from jax.sharding import PartitionSpec as P

GLL_NODES = (
    -1.0,
    -0.8717401485096066,
    -0.5917001814331423,
    -0.2092992179024789,
    0.2092992179024789,
    0.5917001814331423,
    0.8717401485096066,
    1.0,
)
NODE_COUNT = len(GLL_NODES)
SCALES = tuple(
    1.0 / math.prod(GLL_NODES[i] - GLL_NODES[m] for m in range(NODE_COUNT) if m != i)
    for i in range(NODE_COUNT)
)
AXES = ("wide", "narrow")
LANES = 128
ROWS = 8
TABLE_COPIES = 8


def lagrange(position):
    node = lax.broadcasted_iota(jnp.int32, (NODE_COUNT, position.shape[1]), 0)
    result = jnp.full(node.shape, SCALES[0], jnp.float32)
    for i in range(1, NODE_COUNT):
        result = jnp.where(node == i, SCALES[i], result)
    for m in range(NODE_COUNT):
        result = result * jnp.where(node == m, 1.0, position - GLL_NODES[m])
    return result


def pack_kernel(
    coords_hbm,
    element_hbm,
    counts_hbm,
    fields_hbm,
    out_ref,
    table_ref,
    coords_ref,
    element_ref,
    counts_ref,
    input_semaphores,
    table_semaphores,
    *,
    element_count,
):
    pairs = ((coords_hbm, coords_ref), (element_hbm, element_ref), (counts_hbm, counts_ref))
    input_copies = [
        pltpu.make_async_copy(source, target, input_semaphores.at[i])
        for i, (source, target) in enumerate(pairs)
    ]
    share = table_ref.shape[0] // TABLE_COPIES
    table_copies = [
        pltpu.make_async_copy(
            fields_hbm.at[pl.ds(i * share, share), :],
            table_ref.at[pl.ds(i * share, share), :],
            table_semaphores.at[i],
        )
        for i in range(TABLE_COPIES)
    ]
    for copy in input_copies + table_copies:
        copy.start()
    for copy in input_copies:
        copy.wait()
    slots, devices = element_ref.shape
    slot = lax.broadcasted_iota(jnp.int32, (slots, devices), 0)
    element = jnp.where(slot < counts_ref[...], element_ref[...], element_count)
    rows = jnp.concatenate(
        [
            coords_ref[...].reshape(3 * slots, devices),
            element.astype(jnp.float32),
            jnp.zeros(((ROWS - 4) * slots, devices), jnp.float32),
        ],
        axis=0,
    )
    out_ref[...] = rows.T
    for copy in table_copies:
        copy.wait()


def evaluate_kernel(
    query_ref, fields_ref, out_ref, query_rows, result_rows, sent_rows, *, senders, slots
):
    points = senders * slots
    table_rows, columns = fields_ref.shape
    element_count = table_rows // NODE_COUNT
    pairs = NODE_COUNT * NODE_COUNT
    field_count = columns // pairs

    def one_block(first):
        query_rows[:, :senders] = query_ref[pl.ds(first, senders), :].T
        query = jnp.concatenate(
            [query_rows[pl.ds(k, ROWS, stride=slots), :senders] for k in range(slots)], axis=1
        )
        basis_r = lagrange(query[0:1]).astype(jnp.bfloat16).astype(jnp.float32)
        basis_s = lagrange(query[1:2])
        basis_t = lagrange(query[2:3])
        element = query[3:4]
        weights = jnp.concatenate(
            [jnp.where(element == float(e), basis_r, 0.0) for e in range(element_count)], axis=0
        ).astype(jnp.bfloat16)
        tensor_st = jnp.concatenate(
            [basis_s[j : j + 1] * basis_t for j in range(NODE_COUNT)], axis=0
        )
        partial = lax.dot_general(
            fields_ref[...],
            weights,
            (((0,), (0,)), ((), ())),
            preferred_element_type=jnp.float32,
        )
        values = jnp.sum(
            partial.reshape(field_count, pairs, points) * tensor_st[None, :, :], axis=1
        )
        for k in range(slots):
            start = k * senders
            tile = values[:, start // LANES * LANES : start // LANES * LANES + LANES]
            shift = start % LANES
            if shift:
                tile = pltpu.roll(tile, LANES - shift, 1)
            result_rows[pl.ds(k, field_count, stride=slots), :] = tile
        pieces = field_count * slots // LANES
        for piece in range(pieces):
            sent_rows[pl.ds(piece, senders, stride=pieces), :] = result_rows[
                piece * LANES : (piece + 1) * LANES, :
            ].T[:senders]
        out_ref[pl.ds(first * pieces, senders * pieces), :] = sent_rows[...].astype(jnp.bfloat16)

    if query_ref.shape[0] == senders:
        one_block(0)
    else:

        @pl.loop(0, query_ref.shape[0] // senders)
        def _(block):
            one_block(pl.multiple_of(block * senders, senders))


def unpack_kernel(result_ref, out_hbm, arrived_rows, values, semaphores):
    field_count, slots, devices = out_hbm.shape
    pieces = field_count * slots // LANES
    share = field_count // pieces
    arrived_rows[...] = result_ref[...].astype(jnp.float32)
    copies = []
    for piece in range(pieces):
        rows = arrived_rows[pl.ds(piece, devices, stride=pieces), :].T
        part = pl.ds(piece * share, share)
        values[part] = rows.reshape(share, slots, devices).astype(jnp.bfloat16)
        copies.append(
            pltpu.make_async_copy(values.at[part], out_hbm.at[part], semaphores.at[piece])
        )
        copies[-1].start()
    for copy in copies:
        copy.wait()


def exchange(array):
    return lax.all_to_all(array, AXES, split_axis=0, concat_axis=0, tiled=True)


def in_vmem(array):
    return pltpu.with_memory_space_constraint(array, pltpu.VMEM)


def on_device(query_coords, owner_element, pair_counts, fields):
    device_count = lax.axis_size("wide") * lax.axis_size("narrow")
    slots = owner_element.shape[1]
    element_count, node_count, columns = fields.shape
    field_count = columns // (node_count * node_count)
    field_table = fields.reshape(element_count * node_count, columns)
    on_chip = pl.BlockSpec(memory_space=pltpu.VMEM)
    queries = (query_coords[:, 0], owner_element[0], pair_counts)
    sent, table = pl.pallas_call(
        functools.partial(pack_kernel, element_count=element_count),
        out_shape=(
            pltpu.VMEM((device_count, ROWS * slots), jnp.float32),
            pltpu.VMEM(field_table.shape, field_table.dtype),
        ),
        in_specs=[pl.BlockSpec(memory_space=pl.ANY)] * 4,
        out_specs=(on_chip, on_chip),
        scratch_shapes=[
            *(pltpu.VMEM(array.shape, array.dtype) for array in queries),
            pltpu.SemaphoreType.DMA((len(queries),)),
            pltpu.SemaphoreType.DMA((TABLE_COPIES,)),
        ],
        name="pack",
    )(*queries, field_table)
    arrived = exchange(sent)
    senders = math.gcd(device_count, 32)
    pieces = field_count * slots // LANES
    result = pl.pallas_call(
        functools.partial(evaluate_kernel, senders=senders, slots=slots),
        out_shape=pltpu.VMEM((device_count * pieces, LANES), jnp.bfloat16),
        in_specs=[on_chip, on_chip],
        out_specs=on_chip,
        scratch_shapes=[
            pltpu.VMEM((ROWS * slots, LANES), jnp.float32),
            pltpu.VMEM((field_count * slots, LANES), jnp.float32),
            pltpu.VMEM((senders * pieces, LANES), jnp.float32),
        ],
        name="evaluate",
    )(in_vmem(arrived), in_vmem(table))
    returned = exchange(result)
    values = pl.pallas_call(
        unpack_kernel,
        out_shape=jax.ShapeDtypeStruct((field_count, slots, device_count), jnp.bfloat16),
        in_specs=[on_chip],
        out_specs=pl.BlockSpec(memory_space=pl.ANY),
        scratch_shapes=[
            pltpu.VMEM((device_count * pieces, LANES), jnp.float32),
            pltpu.VMEM((field_count, slots, device_count), jnp.bfloat16),
            pltpu.SemaphoreType.DMA((pieces,)),
        ],
        name="unpack",
    )(in_vmem(returned))
    return values[:, None]


def solution(mesh):
    placed = (
        P(None, AXES, None, None),
        P(AXES, None, None),
        P(AXES, None),
        P(AXES, None, None),
    )
    return jax.shard_map(
        on_device,
        mesh=mesh,
        in_specs=placed,
        out_specs=P(None, AXES, None, None),
        check_vma=False,
    )
```
